8 devices in a mesh: dp: 1 (over z), sp: 8 (over x, y, core).
Axes of the slice: x: 2, y: 2, z: 1, core: 2. Of those that a mesh axis runs over, the one named last changes fastest.
Arguments:
- q: bfloat16 [32, 32, 160], P('dp')
- k: bfloat16 [32, 8192, 8, 160], P('dp', 'sp')
- v: bfloat16 [32, 8192, 8, 160], P('dp', 'sp')
Outputs:
- q: bfloat16 [32, 32, 160], P('dp')
All inputs are finite; a program needn't handle non-finite values.
Results may differ from the reference program's by a relative error of at most 0.012.
Values are sent between devices in bfloat16 or wider.
A program may use at most 2 GiB of HBM per device.

```python
import jax
import jax.numpy as jnp

BATCH = 32
CACHE = 8192
HEADS = 32
KV_HEADS = 8
HEAD = 160


def setup_inputs(seed: int = 0, part: int = 0) -> dict:
    kq, kk, kv = (jax.random.fold_in(k, part) for k in jax.random.split(jax.random.key(seed), 3))
    return {
        "q": (3 * jax.random.normal(kq, (BATCH, HEADS, HEAD), jnp.float32)).astype(jnp.bfloat16),
        "k": jax.random.normal(kk, (BATCH, CACHE, KV_HEADS, HEAD), jnp.float32).astype(jnp.bfloat16),
        "v": jax.random.normal(kv, (BATCH, CACHE, KV_HEADS, HEAD), jnp.float32).astype(jnp.bfloat16),
    }


def einsum(form, a, b):
    return jnp.einsum(form, a.astype(jnp.float32), b.astype(jnp.float32))


def reference(q, k, v):
    grouped = q.reshape(BATCH, KV_HEADS, -1, HEAD)
    scores = einsum("bgsd,bugd->bgsu", grouped, k) * HEAD**-0.5
    weights = jax.nn.softmax(scores, -1).astype(jnp.bfloat16)
    return einsum("bgsu,bugd->bgsd", weights, v).astype(jnp.bfloat16).reshape(BATCH, HEADS, HEAD)
```

```python
import functools

import jax
import jax.numpy as jnp
from jax import lax
from jax.experimental import pallas as pl
from jax.experimental.pallas import tpu as pltpu
from jax.sharding import PartitionSpec as P

GROUP = 4
LANES = 128
MESH = pl.DeviceIdType.MESH


def kernel(n, axis, q_hbm, k_hbm, v_hbm, o_ref, q_buf, k_buf, v_buf, weights, highs, totals, parts, stats, q_sem, k_sem, v_sem,
           part_send, part_recv, stat_send, stat_recv):
    seqs, heads, head = q_buf.shape
    wide = k_buf.shape[1]
    kv_heads = wide // head
    share = heads // kv_heads
    rest = head - LANES
    groups = seqs // GROUP
    me = lax.axis_index(axis)

    barrier = pltpu.get_barrier_semaphore()
    for step in range(1, n):
        pl.semaphore_signal(barrier, inc=1, device_id={axis: lax.rem(me + step, n)}, device_id_type=MESH)

    def k_copy(seq, slot):
        return pltpu.make_async_copy(k_hbm.at[seq], k_buf.at[slot], k_sem.at[slot])

    def v_copy(seq, slot):
        return pltpu.make_async_copy(v_hbm.at[seq], v_buf.at[slot], v_sem.at[slot])

    q_copy = pltpu.make_async_copy(q_hbm, q_buf, q_sem)
    q_copy.start()
    for seq in range(GROUP):
        k_copy(seq, seq).start()
        v_copy(seq, seq).start()
    q_copy.wait()

    row = lax.broadcasted_iota(jnp.int32, (heads, wide), 0)
    lane = lax.broadcasted_iota(jnp.int32, (heads, wide), 1)
    first = (row // share) * head
    own = (lane >= first) & (lane < first + head)
    upper = lax.broadcasted_iota(jnp.int32, (2 * share, head), 0) < share
    place = lax.broadcasted_iota(jnp.int32, (heads, LANES), 1)

    def score(seq, slot):
        q = q_buf[seq].astype(jnp.float32)
        spread = jnp.where(own, jnp.concatenate([q] * kv_heads, axis=1), 0.0).astype(jnp.bfloat16)
        scores = jnp.dot(spread, k_buf[slot], preferred_element_type=jnp.float32) * head**-0.5
        high = jnp.max(scores, axis=1, keepdims=True)
        w = jnp.exp(scores - high)
        weights[slot] = w.astype(jnp.bfloat16)
        highs[slot] = jnp.broadcast_to(high, (heads, LANES))
        totals[slot] = jnp.broadcast_to(jnp.sum(w, axis=1, keepdims=True), (heads, LANES))

    def attend(slot):
        seen = lax.dot_general(weights[slot], v_buf[slot], (((1,), (1,)), ((), ())), preferred_element_type=jnp.float32)
        out = []
        for pair in range(kv_heads // 2):
            block = seen[2 * share * pair : 2 * share * (pair + 1), 2 * head * pair : 2 * head * (pair + 1)]
            out.append(jnp.where(upper, block[:, :head], block[:, head:]))
        return jnp.concatenate(out, axis=0)

    def share_out(group):
        for what, send, recv in ((parts, part_send, part_recv), (stats, stat_send, stat_recv)):
            for step in range(1, n):
                pltpu.make_async_remote_copy(
                    src_ref=what.at[group, me],
                    dst_ref=what.at[group, me],
                    send_sem=send,
                    recv_sem=recv.at[group, step - 1],
                    device_id={axis: lax.rem(me + step, n)},
                    device_id_type=MESH,
                ).start()

    def combine(group):
        for step in range(1, n):
            there = lax.rem(me + n - step, n)
            for what, recv in ((parts, part_recv), (stats, stat_recv)):
                ref = what.at[group, there]
                pltpu.make_async_copy(ref, ref, recv.at[group, step - 1]).wait()
        high = [stats[group, d, :GROUP, :] for d in range(n)]
        total = [stats[group, d, GROUP:, :] for d in range(n)]
        top = functools.reduce(jnp.maximum, high)
        scale = [jnp.exp(h - top) for h in high]
        inverse = 1.0 / functools.reduce(jnp.add, [t * s for t, s in zip(total, scale)])
        columns = jnp.transpose(jnp.concatenate([s * inverse for s in scale], axis=0))
        main = [jnp.zeros((heads, LANES), jnp.float32) for _ in range(GROUP)]
        tail = jnp.zeros((heads, LANES), jnp.float32)
        for d in range(n):
            mixed = None
            for j in range(GROUP):
                at = d * GROUP + j
                column = jnp.broadcast_to(columns[:heads, at : at + 1], (heads, LANES))
                main[j] += column * parts[group, d, heads * j : heads * (j + 1), :].astype(jnp.float32)
                mixed = column if mixed is None else jnp.where(place < rest * j, mixed, column)
            tail += mixed * parts[group, d, heads * GROUP :, :].astype(jnp.float32)
        for j in range(GROUP):
            o_ref[group * GROUP + j] = jnp.concatenate([main[j], tail[:, rest * j : rest * (j + 1)]], axis=1).astype(o_ref.dtype)

    def run(group, last):
        tails, table = [], jnp.zeros((heads, LANES), jnp.float32)
        for j in range(GROUP):
            seq, ahead = group * GROUP + j, (j + 1) % GROUP
            scores_next = not (last and j == GROUP - 1)
            if scores_next:
                k_copy(seq + 1, ahead).wait()
            v_copy(seq, j).wait()
            table = jnp.where(place == j, highs[j], table)
            table = jnp.where(place == GROUP + j, totals[j], table)
            if scores_next:
                score(seq + 1, ahead)
            out = attend(j)
            parts[group, me, heads * j : heads * (j + 1), :] = out[:, :LANES].astype(jnp.bfloat16)
            tails.append(out[:, LANES:])
            if not last:
                @pl.when(seq + 1 + GROUP < seqs)
                def _():
                    k_copy(seq + 1 + GROUP, ahead).start()

                v_copy(seq + GROUP, j).start()
        parts[group, me, heads * GROUP :, :] = jnp.concatenate(tails, axis=1).astype(jnp.bfloat16)
        turned = jnp.transpose(table)[: 2 * GROUP, :]
        stats[group, me] = jnp.concatenate([turned, jnp.zeros((2 * GROUP, LANES - heads), jnp.float32)], axis=1)

    k_copy(0, 0).wait()
    score(0, 0)
    k_copy(GROUP, 0).start()
    run(0, False)
    pl.semaphore_wait(barrier, n - 1)
    share_out(0)

    def middle(group, carry):
        run(group, False)
        share_out(group)
        combine(group - 1)
        return carry

    lax.fori_loop(1, groups - 1, middle, 0)
    run(groups - 1, True)
    share_out(groups - 1)
    combine(groups - 2)
    combine(groups - 1)
    for what, send in ((parts, part_send), (stats, stat_send)):
        ref = what.at[:, pl.ds(0, n - 1)]
        pltpu.make_async_copy(ref, ref, send).wait()


def attention(n, axis, q, k, v):
    seqs, run, kv_heads, head = k.shape
    heads = q.shape[1]
    groups = seqs // GROUP
    k, v = (x.transpose(0, 2, 3, 1).reshape(seqs, kv_heads * head, run) for x in (k, v))
    q, k, v = (pltpu.with_memory_space_constraint(x, pltpu.HBM) for x in (q, k, v))
    return pl.pallas_call(
        functools.partial(kernel, n, axis),
        out_shape=jax.ShapeDtypeStruct(q.shape, jnp.bfloat16),
        in_specs=[pl.BlockSpec(memory_space=pltpu.HBM)] * 3,
        out_specs=pl.BlockSpec(memory_space=pltpu.VMEM),
        scratch_shapes=[
            pltpu.VMEM(q.shape, jnp.bfloat16),
            pltpu.VMEM((GROUP, kv_heads * head, run), jnp.bfloat16),
            pltpu.VMEM((GROUP, kv_heads * head, run), jnp.bfloat16),
            pltpu.VMEM((GROUP, heads, run), jnp.bfloat16),
            pltpu.VMEM((GROUP, heads, LANES), jnp.float32),
            pltpu.VMEM((GROUP, heads, LANES), jnp.float32),
            pltpu.VMEM((groups, n, GROUP * heads * head // LANES, LANES), jnp.bfloat16),
            pltpu.VMEM((groups, n, 2 * GROUP, LANES), jnp.float32),
            pltpu.SemaphoreType.DMA,
            pltpu.SemaphoreType.DMA((GROUP,)),
            pltpu.SemaphoreType.DMA((GROUP,)),
            pltpu.SemaphoreType.DMA,
            pltpu.SemaphoreType.DMA((groups, n - 1)),
            pltpu.SemaphoreType.DMA,
            pltpu.SemaphoreType.DMA((groups, n - 1)),
        ],
        compiler_params=pltpu.CompilerParams(collective_id=0, has_side_effects=True, vmem_limit_bytes=48 * 2**20),
    )(q, k, v)


def solution(mesh):
    n = mesh.shape["sp"]
    return jax.shard_map(
        functools.partial(attention, n, "sp"),
        mesh=mesh,
        in_specs=(P("dp", None, None), P("dp", "sp", None, None), P("dp", "sp", None, None)),
        out_specs=P("dp", None, None),
        check_vma=False,
    )
```

```python
import functools

import jax
import jax.numpy as jnp
from jax import lax
from jax.experimental import pallas as pl
from jax.experimental.pallas import tpu as pltpu
from jax.sharding import PartitionSpec as P

GROUP = 4
LANES = 128
MESH = pl.DeviceIdType.MESH


def kernel(n, axis, q_hbm, k_hbm, v_hbm, o_ref, q_buf, k_buf, v_buf, weights, parts, stats, q_sem, k_sem, v_sem,
           part_send, part_recv, late_recv, stat_send, stat_recv):
    seqs, heads, head = q_buf.shape
    wide = k_buf.shape[1]
    kv_heads = wide // head
    share = heads // kv_heads
    fold = LANES // heads
    rows = head // fold
    groups = seqs // GROUP
    me = lax.axis_index(axis)

    barrier = pltpu.get_barrier_semaphore()
    for step in range(1, n):
        pl.semaphore_signal(barrier, inc=1, device_id={axis: lax.rem(me + step, n)}, device_id_type=MESH)

    def k_copy(seq, slot):
        return pltpu.make_async_copy(k_hbm.at[seq], k_buf.at[slot], k_sem.at[slot])

    def v_copy(seq, slot):
        return pltpu.make_async_copy(v_hbm.at[seq], v_buf.at[slot], v_sem.at[slot])

    q_copy = pltpu.make_async_copy(q_hbm, q_buf, q_sem)
    q_copy.start()
    for seq in range(GROUP):
        k_copy(seq, seq).start()
        v_copy(seq, seq).start()
    q_copy.wait()

    row = lax.broadcasted_iota(jnp.int32, (heads, wide), 0)
    lane = lax.broadcasted_iota(jnp.int32, (heads, wide), 1)
    first = (row // share) * head
    own = (lane >= first) & (lane < first + head)
    column = lax.broadcasted_iota(jnp.int32, (heads, LANES), 1)
    of_kv = lax.broadcasted_iota(jnp.int32, (head, heads), 1) // share

    def score(group, slot):
        q = q_buf[group * GROUP + slot].astype(jnp.float32)
        spread = jnp.where(own, jnp.concatenate([q] * kv_heads, axis=1), 0.0).astype(jnp.bfloat16)
        scores = jnp.dot(spread, k_buf[slot], preferred_element_type=jnp.float32) * head**-0.5
        high = jnp.max(scores, axis=1, keepdims=True)
        w = jnp.exp(scores - high)
        weights[slot] = w.astype(jnp.bfloat16)
        turned = jnp.transpose(jnp.where(column == 0, high, jnp.sum(w, axis=1, keepdims=True)))
        stats[group, me, slot] = jnp.concatenate([turned[:2, :]] * fold, axis=1)

    def attend(group, slot):
        w = weights[slot]
        out = None
        for kv in range(kv_heads):
            seen = lax.dot_general(
                v_buf[slot, head * kv : head * (kv + 1), :], w, (((1,), (1,)), ((), ())), preferred_element_type=jnp.float32
            )
            out = seen if out is None else jnp.where(of_kv == kv, seen, out)
        folded = jnp.concatenate([out[rows * f : rows * (f + 1)] for f in range(fold)], axis=1)
        blank = jnp.zeros((parts.shape[3] - rows, LANES), jnp.float32)
        parts[group, me, slot] = jnp.concatenate([folded, blank], axis=0).astype(jnp.bfloat16)

    def spread_out(src, dst, send, recv):
        for step in range(1, n):
            pltpu.make_async_remote_copy(
                src_ref=src,
                dst_ref=dst,
                send_sem=send,
                recv_sem=recv.at[step - 1],
                device_id={axis: lax.rem(me + step, n)},
                device_id_type=MESH,
            ).start()

    def send_part(group, slot, last):
        ref = parts.at[group, me, slot]
        spread_out(ref, ref, part_send, late_recv.at[slot] if last else part_recv.at[group])

    def send_stats(group):
        ref = stats.at[group, me]
        spread_out(ref, ref, stat_send, stat_recv.at[group])

    def arrive(what, recv):
        for step in range(1, n):
            ref = what(lax.rem(me + n - step, n))
            pltpu.make_async_copy(ref, ref, recv.at[step - 1]).wait()

    def combine(group, slot):
        high = [stats[group, d, slot, 0:1, :] for d in range(n)]
        total = [stats[group, d, slot, 1:2, :] for d in range(n)]
        top = functools.reduce(jnp.maximum, high)
        scale = [jnp.exp(h - top) for h in high]
        inverse = 1.0 / functools.reduce(jnp.add, [t * s for t, s in zip(total, scale)])
        out = functools.reduce(
            jnp.add, [parts[group, d, slot, :rows, :].astype(jnp.float32) * (scale[d] * inverse) for d in range(n)]
        )
        turned = jnp.transpose(out)
        o_ref[group * GROUP + slot] = jnp.concatenate(
            [turned[heads * f : heads * (f + 1), :] for f in range(fold)], axis=1
        ).astype(o_ref.dtype)

    def combine_group(group):
        arrive(lambda d: stats.at[group, d], stat_recv.at[group])
        arrive(lambda d: parts.at[group, d], part_recv.at[group])
        for slot in range(GROUP):
            combine(group, slot)

    def run(group, last):
        for slot in range(GROUP):
            seq, ahead = group * GROUP + slot, (slot + 1) % GROUP
            more = not (last and slot == GROUP - 1)
            if more:
                k_copy(seq + 1, ahead).wait()
            v_copy(seq, slot).wait()
            if more:
                score(group + (slot + 1) // GROUP, ahead)
            attend(group, slot)
            if not last:
                @pl.when(seq + 1 + GROUP < seqs)
                def _():
                    k_copy(seq + 1 + GROUP, ahead).start()

                v_copy(seq + GROUP, slot).start()
            if isinstance(group, int) and group == 0 and slot == 0:
                pl.semaphore_wait(barrier, n - 1)
            send_part(group, slot, last)
            if slot == GROUP - 2:
                send_stats(group)

    k_copy(0, 0).wait()
    score(0, 0)
    k_copy(GROUP, 0).start()
    run(0, False)

    def middle(group, carry):
        run(group, False)
        combine_group(group - 1)
        return carry

    lax.fori_loop(1, groups - 1, middle, 0)
    run(groups - 1, True)
    combine_group(groups - 2)
    arrive(lambda d: stats.at[groups - 1, d], stat_recv.at[groups - 1])
    for slot in range(GROUP):
        arrive(lambda d: parts.at[groups - 1, d, slot], late_recv.at[slot])
        combine(groups - 1, slot)
    for what, send in ((parts, part_send), (stats, stat_send)):
        ref = what.at[:, pl.ds(0, n - 1)]
        pltpu.make_async_copy(ref, ref, send).wait()


def attention(n, axis, q, k, v):
    seqs, run, kv_heads, head = k.shape
    heads = q.shape[1]
    groups = seqs // GROUP
    rows = -(-heads * head // LANES // 16) * 16
    k, v = (x.transpose(0, 2, 3, 1).reshape(seqs, kv_heads * head, run) for x in (k, v))
    q, k, v = (pltpu.with_memory_space_constraint(x, pltpu.HBM) for x in (q, k, v))
    return pl.pallas_call(
        functools.partial(kernel, n, axis),
        out_shape=jax.ShapeDtypeStruct(q.shape, jnp.bfloat16),
        in_specs=[pl.BlockSpec(memory_space=pltpu.HBM)] * 3,
        out_specs=pl.BlockSpec(memory_space=pltpu.VMEM),
        scratch_shapes=[
            pltpu.VMEM(q.shape, jnp.bfloat16),
            pltpu.VMEM((GROUP, kv_heads * head, run), jnp.bfloat16),
            pltpu.VMEM((GROUP, kv_heads * head, run), jnp.bfloat16),
            pltpu.VMEM((GROUP, heads, run), jnp.bfloat16),
            pltpu.VMEM((groups, n, GROUP, rows, LANES), jnp.bfloat16),
            pltpu.VMEM((groups, n, GROUP, 2, LANES), jnp.float32),
            pltpu.SemaphoreType.DMA,
            pltpu.SemaphoreType.DMA((GROUP,)),
            pltpu.SemaphoreType.DMA((GROUP,)),
            pltpu.SemaphoreType.DMA,
            pltpu.SemaphoreType.DMA((groups, n - 1)),
            pltpu.SemaphoreType.DMA((GROUP, n - 1)),
            pltpu.SemaphoreType.DMA,
            pltpu.SemaphoreType.DMA((groups, n - 1)),
        ],
        compiler_params=pltpu.CompilerParams(collective_id=0, has_side_effects=True, vmem_limit_bytes=48 * 2**20),
    )(q, k, v)


def solution(mesh):
    n = mesh.shape["sp"]
    return jax.shard_map(
        functools.partial(attention, n, "sp"),
        mesh=mesh,
        in_specs=(P("dp", None, None), P("dp", "sp", None, None), P("dp", "sp", None, None)),
        out_specs=P("dp", None, None),
        check_vma=False,
    )
```

```python
import functools

import jax
import jax.numpy as jnp
from jax import lax
from jax.experimental import pallas as pl
from jax.experimental.pallas import tpu as pltpu
from jax.sharding import PartitionSpec as P

GROUP = 4
LANES = 128
MESH = pl.DeviceIdType.MESH


def kernel(n, axis, q_hbm, k_hbm, v_hbm, o_ref, q_buf, k_buf, v_buf, weights, parts, stats, q_sem, k_sem, v_sem,
           part_send, part_recv, late_recv, stat_send, stat_recv):
    seqs, heads, head = q_buf.shape
    wide = k_buf.shape[1]
    kv_heads = wide // head
    share = heads // kv_heads
    fold = LANES // heads
    rows = head // fold
    groups = seqs // GROUP
    me = lax.axis_index(axis)

    barrier = pltpu.get_barrier_semaphore()
    for step in range(1, n):
        pl.semaphore_signal(barrier, inc=1, device_id={axis: lax.rem(me + step, n)}, device_id_type=MESH)

    def k_copy(seq, slot):
        return pltpu.make_async_copy(k_hbm.at[seq], k_buf.at[slot], k_sem.at[slot])

    def v_copy(seq, slot):
        return pltpu.make_async_copy(v_hbm.at[seq], v_buf.at[slot], v_sem.at[slot])

    q_copy = pltpu.make_async_copy(q_hbm, q_buf, q_sem)
    q_copy.start()
    for seq in range(GROUP):
        k_copy(seq, seq).start()
        v_copy(seq, seq).start()
    q_copy.wait()

    row = lax.broadcasted_iota(jnp.int32, (heads, wide), 0)
    lane = lax.broadcasted_iota(jnp.int32, (heads, wide), 1)
    first = (row // share) * head
    own = (lane >= first) & (lane < first + head)
    column = lax.broadcasted_iota(jnp.int32, (heads, LANES), 1)
    of_kv = lax.broadcasted_iota(jnp.int32, (head, heads), 1) // share

    def score(group, slot):
        q = q_buf[group * GROUP + slot].astype(jnp.float32)
        spread = jnp.where(own, jnp.concatenate([q] * kv_heads, axis=1), 0.0).astype(jnp.bfloat16)
        scores = jnp.dot(spread, k_buf[slot], preferred_element_type=jnp.float32) * head**-0.5
        high = jnp.max(scores, axis=1, keepdims=True)
        w = jnp.exp(scores - high)
        weights[slot] = w.astype(jnp.bfloat16)
        turned = jnp.transpose(jnp.where(column == 0, high, jnp.sum(w, axis=1, keepdims=True)))
        stats[group, me, slot] = jnp.concatenate([turned[:2, :]] * fold, axis=1)

    def attend(group, slot):
        w = weights[slot]
        out = None
        for kv in range(kv_heads):
            seen = lax.dot_general(
                v_buf[slot, head * kv : head * (kv + 1), :], w, (((1,), (1,)), ((), ())), preferred_element_type=jnp.float32
            )
            out = seen if out is None else jnp.where(of_kv == kv, seen, out)
        folded = jnp.concatenate([out[rows * f : rows * (f + 1)] for f in range(fold)], axis=1)
        blank = jnp.zeros((parts.shape[3] - rows, LANES), jnp.float32)
        parts[group, me, slot] = jnp.concatenate([folded, blank], axis=0).astype(jnp.bfloat16)

    def spread_out(src, dst, send, recv):
        for step in range(1, n):
            pltpu.make_async_remote_copy(
                src_ref=src,
                dst_ref=dst,
                send_sem=send,
                recv_sem=recv.at[step - 1],
                device_id={axis: lax.rem(me + step, n)},
                device_id_type=MESH,
            ).start()

    def send_parts(group, first, count, recv):
        ref = parts.at[group, me, pl.ds(first, count)]
        spread_out(ref, ref, part_send, recv)

    def send_stats(group):
        ref = stats.at[group, me]
        spread_out(ref, ref, stat_send, stat_recv.at[group])

    def arrive(what, recv):
        for step in range(1, n):
            ref = what(lax.rem(me + n - step, n))
            pltpu.make_async_copy(ref, ref, recv.at[step - 1]).wait()

    def combine(group, slot):
        high = [stats[group, d, slot, 0:1, :] for d in range(n)]
        total = [stats[group, d, slot, 1:2, :] for d in range(n)]
        top = functools.reduce(jnp.maximum, high)
        scale = [jnp.exp(h - top) for h in high]
        inverse = 1.0 / functools.reduce(jnp.add, [t * s for t, s in zip(total, scale)])
        out = functools.reduce(
            jnp.add, [parts[group, d, slot, :rows, :].astype(jnp.float32) * (scale[d] * inverse) for d in range(n)]
        )
        turned = jnp.transpose(out)
        o_ref[group * GROUP + slot] = jnp.concatenate(
            [turned[heads * f : heads * (f + 1), :] for f in range(fold)], axis=1
        ).astype(o_ref.dtype)

    def arrive_group(group):
        arrive(lambda d: stats.at[group, d], stat_recv.at[group])
        arrive(lambda d: parts.at[group, d], part_recv.at[group])

    def run(group, mix, last=False, start=False):
        for slot in range(GROUP):
            seq, ahead = group * GROUP + slot, (slot + 1) % GROUP
            more = not (last and slot == GROUP - 1)
            if mix and slot == 0:
                arrive_group(group - 2)
            if more:
                k_copy(seq + 1, ahead).wait()
            v_copy(seq, slot).wait()
            if mix:
                combine(group - 2, slot)
            if more:
                score(group + (slot + 1) // GROUP, ahead)
            attend(group, slot)
            if not last:
                @pl.when(seq + 1 + GROUP < seqs)
                def _():
                    k_copy(seq + 1 + GROUP, ahead).start()

                v_copy(seq + GROUP, slot).start()
            if start and slot == 0:
                pl.semaphore_wait(barrier, n - 1)
            if last:
                send_parts(group, slot, 1, late_recv.at[slot])
            elif slot % 2:
                send_parts(group, slot - 1, 2, part_recv.at[group])
            if slot == GROUP - 2:
                send_stats(group)

    k_copy(0, 0).wait()
    score(0, 0)
    k_copy(GROUP, 0).start()
    run(0, False, start=True)
    run(1, False)
    lax.fori_loop(2, groups - 1, lambda group, carry: (run(group, True), carry)[1], 0)
    run(groups - 1, True, last=True)
    arrive_group(groups - 2)
    for slot in range(GROUP):
        combine(groups - 2, slot)
    arrive(lambda d: stats.at[groups - 1, d], stat_recv.at[groups - 1])
    for slot in range(GROUP):
        arrive(lambda d: parts.at[groups - 1, d, slot], late_recv.at[slot])
        combine(groups - 1, slot)
    for what, send in ((parts, part_send), (stats, stat_send)):
        ref = what.at[:, pl.ds(0, n - 1)]
        pltpu.make_async_copy(ref, ref, send).wait()


def attention(n, axis, q, k, v):
    seqs, run, kv_heads, head = k.shape
    heads = q.shape[1]
    groups = seqs // GROUP
    rows = -(-heads * head // LANES // 16) * 16
    k, v = (x.transpose(0, 2, 3, 1).reshape(seqs, kv_heads * head, run) for x in (k, v))
    q, k, v = (pltpu.with_memory_space_constraint(x, pltpu.HBM) for x in (q, k, v))
    return pl.pallas_call(
        functools.partial(kernel, n, axis),
        out_shape=jax.ShapeDtypeStruct(q.shape, jnp.bfloat16),
        in_specs=[pl.BlockSpec(memory_space=pltpu.HBM)] * 3,
        out_specs=pl.BlockSpec(memory_space=pltpu.VMEM),
        scratch_shapes=[
            pltpu.VMEM(q.shape, jnp.bfloat16),
            pltpu.VMEM((GROUP, kv_heads * head, run), jnp.bfloat16),
            pltpu.VMEM((GROUP, kv_heads * head, run), jnp.bfloat16),
            pltpu.VMEM((GROUP, heads, run), jnp.bfloat16),
            pltpu.VMEM((groups, n, GROUP, rows, LANES), jnp.bfloat16),
            pltpu.VMEM((groups, n, GROUP, 2, LANES), jnp.float32),
            pltpu.SemaphoreType.DMA,
            pltpu.SemaphoreType.DMA((GROUP,)),
            pltpu.SemaphoreType.DMA((GROUP,)),
            pltpu.SemaphoreType.DMA,
            pltpu.SemaphoreType.DMA((groups, n - 1)),
            pltpu.SemaphoreType.DMA((GROUP, n - 1)),
            pltpu.SemaphoreType.DMA,
            pltpu.SemaphoreType.DMA((groups, n - 1)),
        ],
        compiler_params=pltpu.CompilerParams(collective_id=0, has_side_effects=True, vmem_limit_bytes=48 * 2**20),
    )(q, k, v)


def solution(mesh):
    n = mesh.shape["sp"]
    return jax.shard_map(
        functools.partial(attention, n, "sp"),
        mesh=mesh,
        in_specs=(P("dp", None, None), P("dp", "sp", None, None), P("dp", "sp", None, None)),
        out_specs=P("dp", None, None),
        check_vma=False,
    )
```

```python
import functools

import jax
import jax.numpy as jnp
from jax import lax
from jax.experimental import pallas as pl
from jax.experimental.pallas import tpu as pltpu
from jax.sharding import PartitionSpec as P

GROUP = 4
LANES = 128
MESH = pl.DeviceIdType.MESH


def kernel(n, axis, q_hbm, k_hbm, v_hbm, o_ref, q_buf, k_buf, v_buf, weights, parts, stats, q_sem, k_sem, v_sem,
           part_send, part_recv, late_recv, stat_send, stat_recv):
    seqs, heads, head = q_buf.shape
    wide = k_buf.shape[1]
    kv_heads = wide // head
    share = heads // kv_heads
    fold = LANES // heads
    rows = head // fold
    groups = seqs // GROUP
    me = lax.axis_index(axis)

    def k_copy(seq, slot):
        return pltpu.make_async_copy(k_hbm.at[seq], k_buf.at[slot], k_sem.at[slot])

    def v_copy(seq, slot):
        return pltpu.make_async_copy(v_hbm.at[seq], v_buf.at[slot], v_sem.at[slot])

    q_copy = pltpu.make_async_copy(q_hbm, q_buf, q_sem)
    k_copy(0, 0).start()
    q_copy.start()
    v_copy(0, 0).start()
    for seq in range(1, GROUP):
        k_copy(seq, seq).start()
        v_copy(seq, seq).start()

    barrier = pltpu.get_barrier_semaphore()
    for step in range(1, n):
        pl.semaphore_signal(barrier, inc=1, device_id={axis: lax.rem(me + step, n)}, device_id_type=MESH)
    q_copy.wait()

    row = lax.broadcasted_iota(jnp.int32, (heads, wide), 0)
    lane = lax.broadcasted_iota(jnp.int32, (heads, wide), 1)
    first = (row // share) * head
    own = (lane >= first) & (lane < first + head)
    column = lax.broadcasted_iota(jnp.int32, (heads, LANES), 1)
    of_kv = lax.broadcasted_iota(jnp.int32, (head, heads), 1) // share

    def score(group, slot):
        q = q_buf[group * GROUP + slot].astype(jnp.float32)
        spread = jnp.where(own, jnp.concatenate([q] * kv_heads, axis=1), 0.0).astype(jnp.bfloat16)
        scores = jnp.dot(spread, k_buf[slot], preferred_element_type=jnp.float32) * head**-0.5
        high = jnp.max(scores, axis=1, keepdims=True)
        w = jnp.exp(scores - high)
        weights[slot] = w.astype(jnp.bfloat16)
        turned = jnp.transpose(jnp.where(column == 0, high, jnp.sum(w, axis=1, keepdims=True)))
        stats[group, me, slot] = jnp.concatenate([turned[:2, :]] * fold, axis=1)

    def attend(group, slot):
        w = weights[slot]
        out = None
        for kv in range(kv_heads):
            seen = lax.dot_general(
                v_buf[slot, head * kv : head * (kv + 1), :], w, (((1,), (1,)), ((), ())), preferred_element_type=jnp.float32
            )
            out = seen if out is None else jnp.where(of_kv == kv, seen, out)
        folded = jnp.concatenate([out[rows * f : rows * (f + 1)] for f in range(fold)], axis=1)
        blank = jnp.zeros((parts.shape[3] - rows, LANES), jnp.float32)
        parts[group, me, slot] = jnp.concatenate([folded, blank], axis=0).astype(jnp.bfloat16)

    peers = sorted(range(1, n), key=lambda bits: (-(bits // 2).bit_count(), bits % 2))

    def spread_out(src, dst, send, recv):
        for at, bits in enumerate(peers):
            pltpu.make_async_remote_copy(
                src_ref=src,
                dst_ref=dst,
                send_sem=send,
                recv_sem=recv.at[at],
                device_id={axis: me ^ bits},
                device_id_type=MESH,
            ).start()

    def send_parts(group, first, count, recv):
        ref = parts.at[group, me, pl.ds(first, count)]
        spread_out(ref, ref, part_send, recv)

    def send_stats(group):
        ref = stats.at[group, me]
        spread_out(ref, ref, stat_send, stat_recv.at[group])

    def arrive(what, recv):
        for at, bits in reversed(list(enumerate(peers))):
            ref = what(me ^ bits)
            pltpu.make_async_copy(ref, ref, recv.at[at]).wait()

    def factors(group, slot):
        high = [stats[group, d, slot, 0:1, :] for d in range(n)]
        total = [stats[group, d, slot, 1:2, :] for d in range(n)]
        top = functools.reduce(jnp.maximum, high)
        scale = [jnp.exp(h - top) for h in high]
        inverse = 1.0 / functools.reduce(jnp.add, [t * s for t, s in zip(total, scale)])
        return [s * inverse for s in scale]

    def combine(group, slot, shares=None):
        shares = shares or factors(group, slot)
        out = functools.reduce(jnp.add, [parts[group, d, slot, :rows, :].astype(jnp.float32) * shares[d] for d in range(n)])
        turned = jnp.transpose(out)
        o_ref[group * GROUP + slot] = jnp.concatenate(
            [turned[heads * f : heads * (f + 1), :] for f in range(fold)], axis=1
        ).astype(o_ref.dtype)

    def arrive_group(group):
        arrive(lambda d: stats.at[group, d], stat_recv.at[group])
        arrive(lambda d: parts.at[group, d], part_recv.at[group])

    def run(group, mix, last=False, start=False):
        for slot in range(GROUP):
            seq, ahead = group * GROUP + slot, (slot + 1) % GROUP
            more = not (last and slot == GROUP - 1)
            if mix and slot == 0:
                arrive_group(group - 2)
            if more:
                k_copy(seq + 1, ahead).wait()
            v_copy(seq, slot).wait()
            if mix:
                combine(group - 2, slot)
            if more:
                score(group + (slot + 1) // GROUP, ahead)
            attend(group, slot)
            if not last:
                @pl.when(seq + 1 + GROUP < seqs)
                def _():
                    k_copy(seq + 1 + GROUP, ahead).start()

                v_copy(seq + GROUP, slot).start()
            if start and slot == 0:
                pl.semaphore_wait(barrier, n - 1)
            if last:
                send_parts(group, slot, 1, late_recv.at[slot])
            elif slot % 2:
                send_parts(group, slot - 1, 2, part_recv.at[group])
            if slot == GROUP - 2:
                send_stats(group)

    k_copy(0, 0).wait()
    score(0, 0)
    k_copy(GROUP, 0).start()
    run(0, False, start=True)
    run(1, False)
    lax.fori_loop(2, groups - 1, lambda group, carry: (run(group, True), carry)[1], 0)
    run(groups - 1, True, last=True)
    arrive_group(groups - 2)
    for slot in range(GROUP):
        combine(groups - 2, slot)
    arrive(lambda d: stats.at[groups - 1, d], stat_recv.at[groups - 1])
    shares = [factors(groups - 1, slot) for slot in range(GROUP)]
    for slot in range(GROUP):
        arrive(lambda d: parts.at[groups - 1, d, slot], late_recv.at[slot])
        combine(groups - 1, slot, shares[slot])
    for what, send in ((parts, part_send), (stats, stat_send)):
        ref = what.at[:, pl.ds(0, n - 1)]
        pltpu.make_async_copy(ref, ref, send).wait()


def attention(n, axis, q, k, v):
    seqs, run, kv_heads, head = k.shape
    heads = q.shape[1]
    groups = seqs // GROUP
    rows = -(-heads * head // LANES // 16) * 16
    k, v = (x.transpose(0, 2, 3, 1).reshape(seqs, kv_heads * head, run) for x in (k, v))
    q, k, v = (pltpu.with_memory_space_constraint(x, pltpu.HBM) for x in (q, k, v))
    return pl.pallas_call(
        functools.partial(kernel, n, axis),
        out_shape=jax.ShapeDtypeStruct(q.shape, jnp.bfloat16),
        in_specs=[pl.BlockSpec(memory_space=pltpu.HBM)] * 3,
        out_specs=pl.BlockSpec(memory_space=pltpu.VMEM),
        scratch_shapes=[
            pltpu.VMEM(q.shape, jnp.bfloat16),
            pltpu.VMEM((GROUP, kv_heads * head, run), jnp.bfloat16),
            pltpu.VMEM((GROUP, kv_heads * head, run), jnp.bfloat16),
            pltpu.VMEM((GROUP, heads, run), jnp.bfloat16),
            pltpu.VMEM((groups, n, GROUP, rows, LANES), jnp.bfloat16),
            pltpu.VMEM((groups, n, GROUP, 2, LANES), jnp.float32),
            pltpu.SemaphoreType.DMA,
            pltpu.SemaphoreType.DMA((GROUP,)),
            pltpu.SemaphoreType.DMA((GROUP,)),
            pltpu.SemaphoreType.DMA,
            pltpu.SemaphoreType.DMA((groups, n - 1)),
            pltpu.SemaphoreType.DMA((GROUP, n - 1)),
            pltpu.SemaphoreType.DMA,
            pltpu.SemaphoreType.DMA((groups, n - 1)),
        ],
        compiler_params=pltpu.CompilerParams(collective_id=0, has_side_effects=True, vmem_limit_bytes=48 * 2**20),
    )(q, k, v)


def solution(mesh):
    n = mesh.shape["sp"]
    return jax.shard_map(
        functools.partial(attention, n, "sp"),
        mesh=mesh,
        in_specs=(P("dp", None, None), P("dp", "sp", None, None), P("dp", "sp", None, None)),
        out_specs=P("dp", None, None),
        check_vma=False,
    )
```

```python
import functools

import jax
import jax.numpy as jnp
from jax import lax
from jax.experimental import pallas as pl
from jax.experimental.pallas import tpu as pltpu
from jax.sharding import PartitionSpec as P

GROUP = 4
LANES = 128
MESH = pl.DeviceIdType.MESH


def kernel(n, axis, q_hbm, k_hbm, v_hbm, o_ref, q_buf, k_buf, v_buf, weights, parts, stats, q_sem, k_sem, v_sem,
           part_send, part_recv, late_recv, stat_send, stat_recv):
    seqs, heads, head = q_buf.shape
    wide = k_buf.shape[1]
    kv_heads = wide // head
    share = heads // kv_heads
    fold = LANES // heads
    rows = head // fold
    groups = seqs // GROUP
    me = lax.axis_index(axis)

    def k_copy(seq, slot):
        return pltpu.make_async_copy(k_hbm.at[seq], k_buf.at[slot], k_sem.at[slot])

    def v_copy(seq, slot):
        return pltpu.make_async_copy(v_hbm.at[seq], v_buf.at[slot], v_sem.at[slot])

    q_copy = pltpu.make_async_copy(q_hbm, q_buf, q_sem)
    k_copy(0, 0).start()
    q_copy.start()
    v_copy(0, 0).start()
    for seq in range(1, GROUP):
        k_copy(seq, seq).start()
        v_copy(seq, seq).start()

    barrier = pltpu.get_barrier_semaphore()
    for step in range(1, n):
        pl.semaphore_signal(barrier, inc=1, device_id={axis: lax.rem(me + step, n)}, device_id_type=MESH)
    q_copy.wait()

    row = lax.broadcasted_iota(jnp.int32, (heads, wide), 0)
    lane = lax.broadcasted_iota(jnp.int32, (heads, wide), 1)
    first = (row // share) * head
    own = (lane >= first) & (lane < first + head)
    column = lax.broadcasted_iota(jnp.int32, (heads, LANES), 1)

    def score(group, slot):
        q = q_buf[group * GROUP + slot].astype(jnp.float32)
        spread = jnp.where(own, jnp.concatenate([q] * kv_heads, axis=1), 0.0).astype(jnp.bfloat16)
        scores = jnp.dot(spread, k_buf[slot], preferred_element_type=jnp.float32) * head**-0.5
        high = jnp.max(scores, axis=1, keepdims=True)
        w = jnp.exp(scores - high)
        weights[slot] = w.astype(jnp.bfloat16)
        turned = jnp.transpose(jnp.where(column == 0, high, jnp.sum(w, axis=1, keepdims=True)))
        stats[group, me, slot] = jnp.concatenate([turned[:2, :]] * fold, axis=1)

    def attend(group, slot, repeat=False):
        w = jnp.concatenate([weights[slot]] * (fold if repeat else 1), axis=0)
        of_kv = lax.broadcasted_iota(jnp.int32, (head, w.shape[0]), 1) % heads // share
        out = None
        for kv in range(kv_heads):
            seen = lax.dot_general(
                v_buf[slot, head * kv : head * (kv + 1), :], w, (((1,), (1,)), ((), ())), preferred_element_type=jnp.float32
            )
            out = seen if out is None else jnp.where(of_kv == kv, seen, out)
        pieces = [out[rows * f : rows * (f + 1)] for f in range(fold)]
        if repeat:
            at = lax.broadcasted_iota(jnp.int32, (rows, LANES), 1) // heads
            folded = functools.reduce(lambda got, f: jnp.where(at == f, pieces[f], got), range(1, fold), pieces[0])
        else:
            folded = jnp.concatenate(pieces, axis=1)
        blank = jnp.zeros((parts.shape[3] - rows, LANES), jnp.float32)
        parts[group, me, slot] = jnp.concatenate([folded, blank], axis=0).astype(jnp.bfloat16)

    peers = sorted(range(1, n), key=lambda bits: (-(bits // 2).bit_count(), bits % 2))

    def spread_out(src, dst, send, recv):
        for at, bits in enumerate(peers):
            pltpu.make_async_remote_copy(
                src_ref=src,
                dst_ref=dst,
                send_sem=send,
                recv_sem=recv.at[at],
                device_id={axis: me ^ bits},
                device_id_type=MESH,
            ).start()

    def send_parts(group, first, count, recv):
        ref = parts.at[group, me, pl.ds(first, count)]
        spread_out(ref, ref, part_send, recv)

    def send_stats(group):
        ref = stats.at[group, me]
        spread_out(ref, ref, stat_send, stat_recv.at[group])

    def arrive(what, recv):
        for at, bits in reversed(list(enumerate(peers))):
            ref = what(me ^ bits)
            pltpu.make_async_copy(ref, ref, recv.at[at]).wait()

    def factors(group, slot):
        high = [stats[group, d, slot, 0:1, :] for d in range(n)]
        total = [stats[group, d, slot, 1:2, :] for d in range(n)]
        top = functools.reduce(jnp.maximum, high)
        scale = [jnp.exp(h - top) for h in high]
        inverse = 1.0 / functools.reduce(jnp.add, [t * s for t, s in zip(total, scale)])
        return [s * inverse for s in scale]

    def combine(group, slot, shares=None):
        shares = shares or factors(group, slot)
        out = functools.reduce(jnp.add, [parts[group, d, slot, :rows, :].astype(jnp.float32) * shares[d] for d in range(n)])
        turned = jnp.transpose(out)
        o_ref[group * GROUP + slot] = jnp.concatenate(
            [turned[heads * f : heads * (f + 1), :] for f in range(fold)], axis=1
        ).astype(o_ref.dtype)

    def arrive_group(group):
        arrive(lambda d: stats.at[group, d], stat_recv.at[group])
        arrive(lambda d: parts.at[group, d], part_recv.at[group])

    def run(group, mix, last=False, start=False):
        for slot in range(GROUP):
            seq, ahead = group * GROUP + slot, (slot + 1) % GROUP
            more = not (last and slot == GROUP - 1)
            if mix and slot == 0:
                arrive_group(group - 2)
            if more:
                k_copy(seq + 1, ahead).wait()
            v_copy(seq, slot).wait()
            if mix:
                combine(group - 2, slot)
            if more:
                score(group + (slot + 1) // GROUP, ahead)
            attend(group, slot, not more)
            if not last:
                @pl.when(seq + 1 + GROUP < seqs)
                def _():
                    k_copy(seq + 1 + GROUP, ahead).start()

                v_copy(seq + GROUP, slot).start()
            if start and slot == 0:
                pl.semaphore_wait(barrier, n - 1)
            if last:
                send_parts(group, slot, 1, late_recv.at[slot])
            elif slot % 2:
                send_parts(group, slot - 1, 2, part_recv.at[group])
            if slot == GROUP - 2:
                send_stats(group)

    k_copy(0, 0).wait()
    score(0, 0)
    k_copy(GROUP, 0).start()
    run(0, False, start=True)
    run(1, False)
    lax.fori_loop(2, groups - 1, lambda group, carry: (run(group, True), carry)[1], 0)
    run(groups - 1, False, last=True)
    for group in (groups - 3, groups - 2):
        arrive_group(group)
        for slot in range(GROUP):
            combine(group, slot)
    arrive(lambda d: stats.at[groups - 1, d], stat_recv.at[groups - 1])
    shares = [factors(groups - 1, slot) for slot in range(GROUP)]
    for slot in range(GROUP):
        arrive(lambda d: parts.at[groups - 1, d, slot], late_recv.at[slot])
        combine(groups - 1, slot, shares[slot])
    for what, send in ((parts, part_send), (stats, stat_send)):
        ref = what.at[:, pl.ds(0, n - 1)]
        pltpu.make_async_copy(ref, ref, send).wait()


def attention(n, axis, q, k, v):
    seqs, run, kv_heads, head = k.shape
    heads = q.shape[1]
    groups = seqs // GROUP
    rows = -(-heads * head // LANES // 16) * 16
    k, v = (x.transpose(0, 2, 3, 1).reshape(seqs, kv_heads * head, run) for x in (k, v))
    q, k, v = (pltpu.with_memory_space_constraint(x, pltpu.HBM) for x in (q, k, v))
    return pl.pallas_call(
        functools.partial(kernel, n, axis),
        out_shape=jax.ShapeDtypeStruct(q.shape, jnp.bfloat16),
        in_specs=[pl.BlockSpec(memory_space=pltpu.HBM)] * 3,
        out_specs=pl.BlockSpec(memory_space=pltpu.VMEM),
        scratch_shapes=[
            pltpu.VMEM(q.shape, jnp.bfloat16),
            pltpu.VMEM((GROUP, kv_heads * head, run), jnp.bfloat16),
            pltpu.VMEM((GROUP, kv_heads * head, run), jnp.bfloat16),
            pltpu.VMEM((GROUP, heads, run), jnp.bfloat16),
            pltpu.VMEM((groups, n, GROUP, rows, LANES), jnp.bfloat16),
            pltpu.VMEM((groups, n, GROUP, 2, LANES), jnp.float32),
            pltpu.SemaphoreType.DMA,
            pltpu.SemaphoreType.DMA((GROUP,)),
            pltpu.SemaphoreType.DMA((GROUP,)),
            pltpu.SemaphoreType.DMA,
            pltpu.SemaphoreType.DMA((groups, n - 1)),
            pltpu.SemaphoreType.DMA((GROUP, n - 1)),
            pltpu.SemaphoreType.DMA,
            pltpu.SemaphoreType.DMA((groups, n - 1)),
        ],
        compiler_params=pltpu.CompilerParams(collective_id=0, has_side_effects=True, vmem_limit_bytes=48 * 2**20),
    )(q, k, v)


def solution(mesh):
    n = mesh.shape["sp"]
    return jax.shard_map(
        functools.partial(attention, n, "sp"),
        mesh=mesh,
        in_specs=(P("dp", None, None), P("dp", "sp", None, None), P("dp", "sp", None, None)),
        out_specs=P("dp", None, None),
        check_vma=False,
    )
```
